32 devices in a mesh: env: 4 (over y, core), dof: 8 (over z, x).
Axes of the slice: x: 2, y: 2, z: 4, core: 2. Of those that a mesh axis runs over, the one named last changes fastest.
Arguments:
- system_matrix: bfloat16 [8, 8192, 8192], P('env', 'dof'), parts along dimension 0, as said below
- forces: float32 [8192, 8, 128], P('dof', 'env'), parts along dimension 1, may hold values from -6 to 6
Outputs:
- accelerations: float32 [8192, 8, 128], P('dof', 'env'), parts along dimension 1
- residual: float32 [8192, 8, 128], P('dof', 'env'), parts along dimension 1
The draws below stay inside these ranges and needn't reach their ends.
There are 4 independent parts, one for each index of `env`. The reference program is written for one: setup_inputs(seed, part) draws one part's arguments, and reference() takes and returns one part's arrays. A program takes and returns all parts, laid end to end along the dimension named above; each array names one. Nothing has to cross between parts.
Inputs may be any that keep to these rules, and one draw needn't show every extreme that they name: `system_matrix`: each environment's matrix is exactly symmetric and positive definite.
All inputs are finite; a program needn't handle non-finite values.
Results may differ from the reference program's by a relative error of at most 0.012.
Values may be sent and summed in bfloat16 or wider, within the bound.
A program may use at most 128 MiB of HBM per device.

```python
import jax
import jax.numpy as jnp
from jax import lax

N = 8192
ENVS = 2
RHS = 128
ITERS = 4


def draw_system_matrix(key, part):
    key_noise = jax.random.fold_in(key, 21)
    key_scale = jax.random.fold_in(key, 22)
    key_shift = jax.random.fold_in(key, 23)
    scales = jnp.exp(jax.random.uniform(key_scale, (ENVS, N), jnp.float32, 0.0, 1.1513))
    shift = jax.random.uniform(key_shift, (ENVS, N), jnp.float32, 0.2, 0.5)

    def one_matrix(index):
        factor = jax.random.normal(jax.random.fold_in(key_noise, index), (N, N), jnp.float32)
        gram = jnp.dot(factor, factor.T, precision=lax.Precision.HIGHEST) * (1.0 / N)
        gram = 0.5 * (gram + gram.T)
        gram = gram + jnp.diag(shift[index])
        outer = scales[index][:, None] * scales[index][None, :]
        return (gram * outer).astype(jnp.bfloat16)
    return lax.map(one_matrix, jnp.arange(ENVS, dtype=jnp.int32))


def levels(stream_key, dims, cuts, least, high):
    level, own = 1.0, jax.random.fold_in(stream_key, 6)
    for dim, blocks in cuts:
        heights = jnp.exp(jax.random.uniform(jax.random.fold_in(own, dim), (blocks,), jnp.float32, least / len(cuts), high / len(cuts)))
        level = level * jnp.repeat(heights, dims[dim] // blocks).reshape([-1 if axis == dim else 1 for axis in range(len(dims))])
    return level


def gaussian(key, dims, scale, reach, pieces=(), kind=jnp.bfloat16):
    array = jax.random.normal(key, dims, jnp.float32) * scale
    if len(pieces) > 0:
        array = levels(key, dims, pieces, -0.22, 0.18) * array
    return jnp.clip(array, min=-reach, max=reach).astype(kind)


def setup_inputs(seed: int = 0, part: int = 0) -> dict:
    splits = jax.random.split(jax.random.key(seed), 3)
    own_keys = jax.random.split(jax.random.fold_in(splits[2], part), 3)
    return {
        "system_matrix": draw_system_matrix(jax.random.fold_in(jax.random.fold_in(splits[2], part), 71), part),
        "forces": gaussian(own_keys[1], (N, ENVS, RHS), 1.0, 6.0, ((0, 8),), jnp.float32),
    }


def apply_matrix(system_matrix, field):
    narrow = field.astype(jnp.bfloat16)
    columns = [jnp.dot(system_matrix[index], narrow[:, index, :], preferred_element_type=jnp.float32) for index in range(ENVS)]
    return jnp.stack(columns, axis=1)


def reference(system_matrix, forces):
    accelerations = jnp.zeros_like(forces)
    residual = forces
    direction = forces
    norm_now = jnp.sum(residual * residual, axis=0)
    for step in range(ITERS):
        image = apply_matrix(system_matrix, direction)
        alpha = norm_now / jnp.sum(direction * image, axis=0)
        accelerations = accelerations + alpha * direction
        residual = residual - alpha * image
        norm_next = jnp.sum(residual * residual, axis=0)
        direction = residual + (norm_next / norm_now) * direction
        norm_now = norm_next
    return accelerations, residual
```

```python
import functools

import jax
import jax.numpy as jnp
from jax import lax
from jax.experimental import pallas as pl
from jax.experimental.pallas import tpu as pltpu
from jax.sharding import PartitionSpec as P

ITERS = 4
MESH = pl.DeviceIdType.MESH


def ring_order(n):
    width = 1
    while (2 * width) ** 2 <= n:
        width *= 2
    depth = n // width
    if width == 1 or depth % 2:
        return list(range(n))
    order = [z * width for z in range(depth)]
    for turn, z in enumerate(reversed(range(depth))):
        xs = list(range(1, width))
        order += [z * width + x for x in (xs if turn % 2 == 0 else xs[::-1])]
    return order


def lookup(table, index):
    value = jnp.int32(0)
    for place, entry in enumerate(table):
        value = value + jnp.where(index == place, jnp.int32(entry), jnp.int32(0))
    return value

PIECES = 4
LADDER = (2, 4)
GATHER = (
    (1, 2, 50, 145, 26, 137, 3, 36, 25, 43, 44, 52, 19, 60, 5, 38, 46, 27, 10, 13, 30, 22, 21, 23, 29, 31, 7, 15),
    (160, 67, 100, 136, 75, 108, 116, 184, 219, 92, 102, 5, 144, 110, 145, 149, 126, 29, 1, 9, 86, 13, 87, 19, 95, 25, 7, 15),
)
SCATTER = (
    (7, 15, 535, 543, 5, 10, 13, 21, 534, 29, 542, 515, 19, 539, 1, 514, 25, 538, 137, 550, 558, 548, 555, 556, 564, 145, 572, 562),
    (7, 15, 531, 1, 5, 265, 13, 25, 541, 149, 599, 95, 598, 67, 401, 614, 638, 400, 622, 219, 612, 416, 440, 75, 620, 392, 628, 604),
)
OWN_SEND = ((5, 5, 5, 5), (7, 5, 6, 7))
OWN_TAKE = ((5, 5, 5, 5), (7, 5, 6, 7))
LEAVES = (18, 8)
GATHER_TURN = 20
SCATTER_TURN = 28
GROUP = 4


def ring_kernel(n, envs, rows, a_hbm, f_ref, x_ref, r_ref, a_vmem, field, direction, image, sums,
           load_sem, send_sem, recv_sem, sum_send, sum_recv):
    order = ring_order(n)
    inverse = [order.index(i) for i in range(n)]
    me = lax.axis_index("dof")
    place = lookup(inverse, me)
    half = rows // 2
    far = n // 2
    tile = min(128, rows)

    def owner(step):
        return lookup(order, lax.rem(place + step + n, n))

    following, previous = owner(1), owner(-1)

    def load(env, block):
        return pltpu.make_async_copy(
            a_hbm.at[env, :, pl.ds(pl.multiple_of(block * rows, rows), rows)],
            a_vmem.at[env, block],
            load_sem.at[env, block],
        )

    def hop(env, way, block, part, target):
        return pltpu.make_async_remote_copy(
            src_ref=field.at[env, block, part],
            dst_ref=field.at[env, block, part],
            send_sem=send_sem.at[env, way, block, part],
            recv_sem=recv_sem.at[env, block, part],
            device_id={"dof": target},
            device_id_type=MESH,
        )

    def forward(env, block, part):
        return hop(env, 0, block, part, following)

    def backward(env, block, part):
        return hop(env, 1, block, part, previous)

    def share(env, slot, peer, source):
        return pltpu.make_async_remote_copy(
            src_ref=sums.at[env, slot, source],
            dst_ref=sums.at[env, slot, source],
            send_sem=sum_send.at[env, slot, peer],
            recv_sem=sum_recv.at[env, slot, source],
            device_id={"dof": peer},
            device_id_type=MESH,
        )

    def peer_of(j):
        return lax.rem(me + j, n)

    def add(env, block, part, first=False):
        product = jnp.dot(
            a_vmem[env, block, :, part * half:(part + 1) * half],
            field[env, block, part],
            preferred_element_type=jnp.float32,
        )
        if first:
            image[env] = product
        else:
            image[env] += product

    def start_own(env):
        for q in range(2):
            forward(env, me, q).start()
            backward(env, me, 1 - q).start()

    def begin(env, k):
        @pl.when(k == 0)
        def _():
            load(env, me).wait()
        add(env, me, 0, first=True)
        add(env, me, 1)

    def near(env, k, s, relay):
        before, after = owner(-s), owner(s)
        for q in range(2):
            forward(env, before, q).wait_recv()
            if relay > q:
                forward(env, before, q).start()
            backward(env, after, 1 - q).wait_recv()
            if relay > q:
                backward(env, after, 1 - q).start()
            if q == 0:
                @pl.when(k == 0)
                def _():
                    load(env, before).wait()
                    load(env, after).wait()
            if relay == 1 and q == 0:
                yield
            add(env, before, q)
            add(env, after, 1 - q)

    def gather(env, k, between):
        begin(env, k)

        def step(s, carry):
            for _ in near(env, k, s, 2):
                pass
            return carry

        lax.fori_loop(1, far - 1, step, 0)
        for _ in near(env, k, far - 1, 1):
            between()
        block = owner(far)
        forward(env, block, 0).wait_recv()

        @pl.when(k == 0)
        def _():
            load(env, block).wait()
        add(env, block, 0)
        backward(env, block, 1).wait_recv()
        add(env, block, 1)

        def drain(s, carry):
            for q in range(2):
                forward(env, owner(-s), q).wait_send()
                backward(env, owner(s), q).wait_send()
            return carry

        lax.fori_loop(0, far - 1, drain, 0)
        forward(env, owner(1 - far), 0).wait_send()
        backward(env, owner(far - 1), 1).wait_send()

    def local_sums(env, k):
        slot = lax.rem(k, 2)

        def step(i, carry):
            at = pl.ds(pl.multiple_of(i * tile, tile), tile)
            r, d, q = r_ref[env, at, :], direction[env, at, :], image[env, at, :]
            fold = lambda v: jnp.sum(v.reshape(tile // 8, 8, v.shape[-1]), axis=0)
            return tuple(c + fold(v) for c, v in zip(carry, (r * r, d * q, r * q, q * q)))

        zero = jnp.zeros((8, image.shape[-1]), jnp.float32)
        totals = lax.fori_loop(0, rows // tile, step, (zero,) * 4)
        for i, total in enumerate(totals):
            sums[env, slot, me, i:i + 1, :] = jnp.sum(total, axis=0, keepdims=True)

        def send(j, carry):
            share(env, slot, peer_of(j), me).start()
            return carry

        lax.fori_loop(1, n, send, 0)

    def update(env, k):
        slot = lax.rem(k, 2)

        def receive(j, carry):
            share(env, slot, me, peer_of(j)).wait_recv()
            share(env, slot, peer_of(j), me).wait_send()
            return carry

        lax.fori_loop(1, n, receive, 0)
        total = sums[env, slot, 0]
        for j in range(1, n):
            total = total + sums[env, slot, j]
        now, curve, cross, square = (total[i:i + 1, :] for i in range(4))
        alpha = now / curve
        beta = (now - 2.0 * alpha * cross + alpha * alpha * square) / now

        def step(i, carry):
            at = pl.ds(pl.multiple_of(i * tile, tile), tile)
            d = direction[env, at, :]
            x_ref[env, at, :] = x_ref[env, at, :] + alpha * d
            r = r_ref[env, at, :] - alpha * image[env, at, :]
            r_ref[env, at, :] = r
            d = r + beta * d
            direction[env, at, :] = d
            put(env, i, d)
            return carry

        lax.fori_loop(0, rows // tile, step, 0)

    def put(env, i, d):
        per = half // tile if half >= tile else 1
        narrow = d.astype(field.dtype)
        if half >= tile:
            at = pl.ds(pl.multiple_of(lax.rem(i, per) * tile, tile), tile)
            field[env, me, i // per, at, :] = narrow
        else:
            for q in range(2):
                field[env, me, q] = narrow[q * half:(q + 1) * half]

    barrier = pltpu.get_barrier_semaphore()

    def greet(j, carry):
        pl.semaphore_signal(barrier, inc=1, device_id={"dof": peer_of(j)}, device_id_type=MESH)
        return carry

    def copy_in(env):
        def step(i, carry):
            at = pl.ds(pl.multiple_of(i * tile, tile), tile)
            f = f_ref[env, at, :]
            x_ref[env, at, :] = jnp.zeros_like(f)
            r_ref[env, at, :] = f
            direction[env, at, :] = f
            put(env, i, f)
            return carry
        lax.fori_loop(0, rows // tile, step, 0)

    lax.fori_loop(1, n, greet, 0)
    copy_in(0)
    for env in range(envs):
        load(env, me).start()

        def fetch(s, carry):
            load(env, owner(-s)).start()
            load(env, owner(s)).start()
            return carry

        lax.fori_loop(1, far, fetch, 0)
        load(env, owner(far)).start()
    pl.semaphore_wait(barrier, n - 1)
    start_own(0)
    copy_in(1)

    def iteration(k, carry):
        def second():
            @pl.when(k > 0)
            def _():
                update(1, k - 1)
            start_own(1)

        def first():
            update(0, k)

            @pl.when(k < ITERS - 1)
            def _():
                start_own(0)

        gather(0, k, second)
        local_sums(0, k)
        gather(1, k, first)
        local_sums(1, k)
        return carry

    lax.fori_loop(0, ITERS, iteration, 0)
    update(1, ITERS - 1)


def ladder_kernel(n, depth, rows, a_hbm, f_ref, x_out, r_out, a_gather, a_scatter,
                  field, inbox, outbox, narrow, parts, xg, rg, dg, image, xs, rs, ds, drawn, sums,
                  load_sem, gather_send, gather_recv, scatter_send, scatter_recv, sum_send, sum_recv):
    width = 2
    rhs = image.shape[-1]
    piece = rows // PIECES
    tile = min(128, rows)
    me = lax.axis_index("dof")
    core = lax.rem(lax.axis_index("env"), 2)
    other = 1 - core
    x = lax.rem(me, width)
    z = me // width
    high = z // (depth // 2)
    place = z + high * (depth - 1 - 2 * z)
    inward = 1 - 2 * high
    targets = (me + 1 - 2 * x, me - width * inward, me + width * inward)
    near_slot, far_slot = (3 - inward) // 2, (3 + inward) // 2
    take_slot = (jnp.int32(0), near_slot, far_slot)
    give_slot = (jnp.int32(0), far_slot, near_slot)

    def by_place(pair):
        return jnp.where(place == 1, jnp.int32(pair[1]), jnp.int32(pair[0]))

    def node(r):
        level = r // width
        return (level + high * (depth - 1 - 2 * level)) * width + lax.rem(x + lax.rem(r, width), width)

    plans = [
        [by_place([t[i] + 1024 * t[i + 1] for t in tables]) for i in range(0, len(tables[0]), 2)]
        for tables in (GATHER, SCATTER)
    ]

    def read_plan(kind, pair):
        word = jnp.int32(0)
        for spot, value in enumerate(plans[kind]):
            word = word + jnp.where(pair == spot, value, jnp.int32(0))
        return [
            (node(lax.rem(entry, 8)), lax.rem(entry // 8, 4), lax.rem(entry // 32, 8), entry // 256)
            for entry in (lax.rem(word, 1024), word // 1024)
        ]

    def for_bits(mask, body):
        for d in range(3):
            @pl.when(lax.rem(mask // (1 << d), 2) == 1)
            def _(d=d):
                body(d)

    def load(kind, block, q):
        env, buffer = ((core, a_gather), (other, a_scatter))[kind]
        return pltpu.make_async_copy(
            a_hbm.at[env, :, pl.ds(pl.multiple_of(block * rows + q * piece, piece), piece)],
            buffer.at[block, q],
            load_sem.at[kind, block, q],
        )

    def spread(block, q, d, k):
        return pltpu.make_async_remote_copy(
            src_ref=field.at[lax.rem(k, 2), block, q],
            dst_ref=field.at[lax.rem(k, 2), block, q],
            send_sem=gather_send.at[block, q, d],
            recv_sem=gather_recv.at[block, q],
            device_id={"dof": targets[d]},
            device_id_type=MESH,
        )

    def collect(block, q, slot, target):
        return pltpu.make_async_remote_copy(
            src_ref=outbox.at[block, q],
            dst_ref=inbox.at[block, q, slot],
            send_sem=scatter_send.at[block, q],
            recv_sem=scatter_recv.at[block, q, slot],
            device_id={"dof": target},
            device_id_type=MESH,
        )

    def share(kind, peer, source):
        return pltpu.make_async_remote_copy(
            src_ref=sums.at[kind, source],
            dst_ref=sums.at[kind, source],
            send_sem=sum_send.at[kind, peer],
            recv_sem=sum_recv.at[kind, source],
            device_id={"dof": peer},
            device_id_type=MESH,
        )

    def peer_of(j):
        return lax.rem(me + j, n)

    def send_field(block, q, mask, k):
        def one(d):
            @pl.when(k > 0)
            def _():
                spread(block, q, d, k - 1).wait_send()
            spread(block, q, d, k).start()
        for_bits(mask, one)

    def gather_start(k):
        for q in range(PIECES):
            send_field(me, q, by_place([t[q] for t in OWN_SEND]), k)

    def loaded(kind, blocks, k):
        @pl.when(k == 0)
        def _():
            for block, q in blocks:
                load(kind, block, q).wait()

    def times(block, q, k):
        return jnp.dot(a_gather[block, q], field[lax.rem(k, 2), block, q], preferred_element_type=jnp.float32)

    def gather_own(k):
        loaded(0, [(me, q) for q in range(PIECES)], k)
        image[...] = functools.reduce(jnp.add, [times(me, q, k) for q in range(PIECES)])

    def gather_steps(lo, hi, k):
        def group(g, carry):
            blocks = []
            for j in range(GROUP // 2):
                for block, q, mask, _ in read_plan(0, g * (GROUP // 2) + j):
                    spread(block, q, 0, k).wait_recv()
                    send_field(block, q, mask, k)
                    blocks.append((block, q))
            loaded(0, blocks, k)
            products = [times(block, q, k) for block, q in blocks]
            image[...] += functools.reduce(jnp.add, products)
            return carry

        lax.fori_loop(lo // GROUP, hi // GROUP, group, 0)

    def gather_drain():
        for q in range(PIECES):
            for_bits(by_place([t[q] for t in OWN_SEND]), lambda d: spread(me, q, d, ITERS - 1).wait_send())

        def step(i, carry):
            for block, q, mask, _ in read_plan(0, i):
                for_bits(mask, lambda d: spread(block, q, d, ITERS - 1).wait_send())
            return carry

        lax.fori_loop(0, len(GATHER[0]) // 2, step, 0)

    def part(block, q):
        return jnp.dot(narrow[...], a_scatter[block, q], preferred_element_type=jnp.float32)

    def take(block, q, mask, total):
        def one(d):
            collect(block, q, take_slot[d], me).wait_recv()
            total[...] += inbox[block, q, take_slot[d]].astype(jnp.float32)
        for_bits(mask, one)

    def give(block, q, parent, value, k):
        @pl.when(k > 0)
        def _():
            collect(block, q, 0, targets[0]).wait_send()
        outbox[block, q] = value.astype(outbox.dtype)
        for d in range(3):
            @pl.when(parent == d)
            def _(d=d):
                collect(block, q, give_slot[d], targets[d]).start()

    def scatter_leaves(k):
        def group(g, carry):
            entries = read_plan(1, g)
            loaded(1, [(block, q) for block, q, _, _ in entries], k)
            values = [part(block, q) for block, q, _, _ in entries]
            for (block, q, _, parent), value in zip(entries, values):
                give(block, q, parent, value, k)
            return carry

        lax.fori_loop(0, leaves // 2, group, 0)

    def scatter_parts(k):
        def group(g, carry):
            entries = read_plan(1, g)
            loaded(1, [(block, q) for block, q, _, _ in entries], k)
            for j, (block, q, _, _) in enumerate(entries):
                parts[2 * g + j] = part(block, q)
            return carry

        lax.fori_loop(leaves // 2, len(SCATTER[0]) // 2, group, 0)
        loaded(1, [(me, q) for q in range(PIECES)], k)
        for q in range(PIECES):
            drawn[q] = part(me, q)

    def scatter_steps(lo, hi, k):
        def step(i, carry):
            for j, (block, q, mask, parent) in enumerate(read_plan(1, i)):
                take(block, q, mask, parts.at[2 * i + j])
                give(block, q, parent, parts[2 * i + j], k)
            return carry

        lax.fori_loop(lo // 2, hi // 2, step, 0)

    def scatter_own():
        for q in range(PIECES):
            take(me, q, by_place([t[q] for t in OWN_TAKE]), drawn.at[q])

    def scatter_drain():
        def step(i, carry):
            for block, q, _, _ in read_plan(1, i):
                collect(block, q, 0, targets[0]).wait_send()
            return carry

        lax.fori_loop(0, len(SCATTER[0]) // 2, step, 0)

    def send_sums(kind, rows_of):
        for i, total in enumerate(rows_of):
            sums[kind, me, i:i + 1, :] = total

        def send(j, carry):
            share(kind, peer_of(j), me).start()
            return carry

        lax.fori_loop(1, n, send, 0)

    def gather_sums():
        def step(i, carry):
            at = pl.ds(pl.multiple_of(i * tile, tile), tile)
            r, d, q = rg[at, :], dg[at, :], image[at, :]
            fold = lambda v: jnp.sum(v.reshape(tile // 8, 8, rhs), axis=0)
            return tuple(c + fold(v) for c, v in zip(carry, (r * r, d * q, r * q, q * q)))

        zero = jnp.zeros((8, rhs), jnp.float32)
        totals = lax.fori_loop(0, rows // tile, step, (zero,) * 4)
        send_sums(0, [jnp.sum(total, axis=0, keepdims=True) for total in totals])

    def cuts():
        for q in range(PIECES):
            for j in range(piece // rhs):
                yield q, slice(j * rhs, (j + 1) * rhs), q * piece + j * rhs

    def scatter_sums():
        totals = [jnp.zeros((rhs, rhs), jnp.float32)] * 4
        for q, lanes, _ in cuts():
            r, d, v = rs[q, :, lanes], ds[q, :, lanes], drawn[q, :, lanes]
            totals = [c + w for c, w in zip(totals, (r * r, d * v, r * v, v * v))]
        send_sums(1, [jnp.sum(total.T, axis=0, keepdims=True) for total in totals])

    def ratios(kind):
        def receive(j, carry):
            share(kind, me, peer_of(j)).wait_recv()
            share(kind, peer_of(j), me).wait_send()
            return carry

        lax.fori_loop(1, n, receive, 0)
        total = sums[kind, 0]
        for j in range(1, n):
            total = total + sums[kind, j]
        now, curve, cross, square = (total[i:i + 1, :] for i in range(4))
        alpha = now / curve
        beta = (now - 2.0 * alpha * cross + alpha * alpha * square) / now
        return alpha, beta

    def gather_update(later):
        alpha, beta = ratios(0)
        for q in range(PIECES):
            at = slice(q * piece, (q + 1) * piece)
            d = dg[at, :]
            xg[at, :] = xg[at, :] + alpha * d
            r = rg[at, :] - alpha * image[at, :]
            rg[at, :] = r
            d = r + beta * d
            dg[at, :] = d
            field[lax.rem(later, 2), me, q] = d.astype(field.dtype)

    def scatter_update():
        alpha, beta = (jnp.broadcast_to(v, (rhs, rhs)).T for v in ratios(1))
        for q, lanes, at in cuts():
            d = ds[q, :, lanes]
            xs[q, :, lanes] = xs[q, :, lanes] + alpha * d
            r = rs[q, :, lanes] - alpha * drawn[q, :, lanes]
            rs[q, :, lanes] = r
            d = r + beta * d
            ds[q, :, lanes] = d
            narrow[:, at:at + rhs] = d.astype(narrow.dtype)

    def strided(env, start, size):
        return pl.ds(env + 2 * start, size, stride=2)

    barrier = pltpu.get_barrier_semaphore()

    def greet(j, carry):
        pl.semaphore_signal(barrier, inc=1, device_id={"dof": peer_of(j)}, device_id_type=MESH)
        return carry

    lax.fori_loop(1, n, greet, 0)
    leaves = by_place(LEAVES)

    def fetch(kind, i):
        block = node(i if kind == 0 else n - 1 - i)
        for q in range(PIECES):
            load(kind, block, q).start()

    def fetch_all(first):
        def body(i, carry):
            fetch(first, i)
            return carry

        lax.fori_loop(0, n, body, 0)

    @pl.when(core == 0)
    def _():
        fetch_all(0)
        fetch_all(1)

    @pl.when(core == 1)
    def _():
        fetch_all(1)
        fetch_all(0)

    for q in range(PIECES):
        at = slice(q * piece, (q + 1) * piece)
        f = f_ref[strided(core, q * piece, piece), :]
        xg[at, :] = jnp.zeros_like(f)
        rg[at, :] = f
        dg[at, :] = f
        field[0, me, q] = f.astype(field.dtype)
    for q, lanes, at in cuts():
        f = f_ref[strided(other, at, rhs), :].T
        xs[q, :, lanes] = jnp.zeros_like(f)
        rs[q, :, lanes] = f
        ds[q, :, lanes] = f
        narrow[:, at:at + rhs] = f.astype(narrow.dtype)

    pl.semaphore_wait(barrier, n - 1)
    turns = 2 * ITERS

    @pl.when(core == 0)
    def _():
        gather_start(jnp.int32(0))
        gather_own(jnp.int32(0))

    @pl.when(core == 1)
    def _():
        scatter_leaves(jnp.int32(0))

    def phase(t, carry):
        k, later = t // 2, (t + 1) // 2
        kind = lax.rem(t + core, 2)

        @pl.when(kind == 0)
        def _():
            gather_steps(0, GATHER_TURN, k)

            @pl.when(t > 0)
            def _():
                scatter_update()

            @pl.when(t < turns - 1)
            def _():
                scatter_leaves(later)
            gather_steps(GATHER_TURN, len(GATHER[0]), k)
            gather_sums()

        @pl.when(kind == 1)
        def _():
            scatter_parts(k)
            scatter_steps(leaves, SCATTER_TURN, k)

            @pl.when(t > 0)
            def _():
                gather_update(later)

            @pl.when(t < turns - 1)
            def _():
                gather_start(later)
                gather_own(later)
            scatter_steps(SCATTER_TURN, len(SCATTER[0]), k)
            scatter_own()
            scatter_sums()
        return carry

    lax.fori_loop(0, turns, phase, 0)
    gather_drain()
    scatter_drain()

    @pl.when(core == 0)
    def _():
        scatter_update()

    @pl.when(core == 1)
    def _():
        gather_update(jnp.int32(ITERS))
    x_out[strided(core, 0, rows), :] = xg[...]
    r_out[strided(core, 0, rows), :] = rg[...]
    for q, lanes, at in cuts():
        x_out[strided(other, at, rhs), :] = xs[q, :, lanes].T
        r_out[strided(other, at, rhs), :] = rs[q, :, lanes].T


def ladder(n, depth, system_matrix, forces):
    envs, rows, _ = system_matrix.shape
    rhs = forces.shape[-1]
    piece = rows // PIECES
    flat = jax.ShapeDtypeStruct((rows * envs, rhs), jnp.float32)
    vmem = pl.BlockSpec(memory_space=pltpu.VMEM)
    tall = pltpu.VMEM((rows, rhs), jnp.float32)
    wide = pltpu.VMEM((PIECES, rhs, piece), jnp.float32)
    x, r = pl.pallas_call(
        functools.partial(ladder_kernel, n, depth, rows),
        out_shape=(flat, flat),
        in_specs=[pl.BlockSpec(memory_space=pl.ANY), vmem],
        out_specs=(vmem, vmem),
        scratch_shapes=[
            pltpu.VMEM((n, PIECES, rows, piece), jnp.bfloat16),
            pltpu.VMEM((n, PIECES, rows, piece), jnp.bfloat16),
            pltpu.VMEM((2, n, PIECES, piece, rhs), jnp.bfloat16),
            pltpu.VMEM((n, PIECES, 3, rhs, piece), jnp.bfloat16),
            pltpu.VMEM((n, PIECES, rhs, piece), jnp.bfloat16),
            pltpu.VMEM((rhs, rows), jnp.bfloat16),
            pltpu.VMEM((len(SCATTER[0]), rhs, piece), jnp.float32),
            tall, tall, tall, tall,
            wide, wide, wide, wide,
            pltpu.VMEM((2, n, 4, rhs), jnp.float32),
            pltpu.SemaphoreType.DMA((2, n, PIECES)),
            pltpu.SemaphoreType.DMA((n, PIECES, 3)),
            pltpu.SemaphoreType.DMA((n, PIECES)),
            pltpu.SemaphoreType.DMA((n, PIECES)),
            pltpu.SemaphoreType.DMA((n, PIECES, 3)),
            pltpu.SemaphoreType.DMA((2, n)),
            pltpu.SemaphoreType.DMA((2, n)),
        ],
        compiler_params=pltpu.CompilerParams(
            collective_id=0, has_side_effects=True, vmem_limit_bytes=62 * 1024 * 1024
        ),
    )(system_matrix, forces.reshape(rows * envs, rhs))
    return x.reshape(rows, envs, rhs), r.reshape(rows, envs, rhs)


def ring(n, system_matrix, forces):
    envs, rows, _ = system_matrix.shape
    rhs = forces.shape[-1]
    block = jax.ShapeDtypeStruct((envs, rows, rhs), jnp.float32)
    vmem = pl.BlockSpec(memory_space=pltpu.VMEM)
    x, r = pl.pallas_call(
        functools.partial(ring_kernel, n, envs, rows),
        out_shape=(block, block),
        in_specs=[pl.BlockSpec(memory_space=pl.ANY), vmem],
        out_specs=(vmem, vmem),
        scratch_shapes=[
            pltpu.VMEM((envs, n, rows, rows), jnp.bfloat16),
            pltpu.VMEM((envs, n, 2, rows // 2, rhs), jnp.bfloat16),
            pltpu.VMEM((envs, rows, rhs), jnp.float32),
            pltpu.VMEM((envs, rows, rhs), jnp.float32),
            pltpu.VMEM((envs, 2, n, 4, rhs), jnp.float32),
            pltpu.SemaphoreType.DMA((envs, n)),
            pltpu.SemaphoreType.DMA((envs, 2, n, 2)),
            pltpu.SemaphoreType.DMA((envs, n, 2)),
            pltpu.SemaphoreType.DMA((envs, 2, n)),
            pltpu.SemaphoreType.DMA((envs, 2, n)),
        ],
        compiler_params=pltpu.CompilerParams(
            collective_id=0, has_side_effects=True, vmem_limit_bytes=60 * 1024 * 1024
        ),
    )(system_matrix, forces.transpose(1, 0, 2))
    return x.transpose(1, 0, 2), r.transpose(1, 0, 2)


def grid_of(n):
    width = 1
    while (2 * width) ** 2 <= n:
        width *= 2
    return width, n // width


def solution(mesh):
    n = mesh.shape["dof"]

    def on_device(system_matrix, forces):
        envs, rows, _ = system_matrix.shape
        rhs = forces.shape[-1]
        fits = envs == 2 and rhs == 128 and rows % (PIECES * rhs) == 0
        if grid_of(n) == LADDER and mesh.shape["env"] % 2 == 0 and fits:
            return ladder(n, LADDER[1], system_matrix, forces)
        return ring(n, system_matrix, forces)

    return jax.shard_map(
        on_device,
        mesh=mesh,
        in_specs=(P("env", "dof", None), P("dof", "env", None)),
        out_specs=(P("dof", "env", None), P("dof", "env", None)),
        check_vma=False,
    )
```

```python
import functools

import jax
import jax.numpy as jnp
from jax import lax
from jax.experimental import pallas as pl
from jax.experimental.pallas import tpu as pltpu
from jax.sharding import PartitionSpec as P

ITERS = 4
MESH = pl.DeviceIdType.MESH


def ring_order(n):
    width = 1
    while (2 * width) ** 2 <= n:
        width *= 2
    depth = n // width
    if width == 1 or depth % 2:
        return list(range(n))
    order = [z * width for z in range(depth)]
    for turn, z in enumerate(reversed(range(depth))):
        xs = list(range(1, width))
        order += [z * width + x for x in (xs if turn % 2 == 0 else xs[::-1])]
    return order


def lookup(table, index):
    value = jnp.int32(0)
    for place, entry in enumerate(table):
        value = value + jnp.where(index == place, jnp.int32(entry), jnp.int32(0))
    return value

PIECES = 4
LADDER = (2, 4)
GATHER = (
    (34, 137, 50, 145, 58, 36, 3, 12, 19, 43, 60, 27, 20, 38, 5, 54, 10, 62, 1, 29, 13, 7, 14, 21, 23, 31, 25, 15),
    (160, 131, 68, 75, 108, 144, 116, 19, 184, 124, 70, 193, 136, 118, 137, 77, 126, 17, 85, 5, 78, 89, 79, 7, 27, 29, 23, 31),
)
SCATTER = (
    (7, 527, 23, 31, 513, 5, 10, 525, 526, 533, 537, 29, 3, 524, 19, 532, 27, 145, 550, 566, 574, 546, 548, 555, 572, 137, 562, 570),
    (519, 23, 31, 517, 273, 29, 19, 27, 193, 131, 591, 77, 590, 393, 85, 392, 89, 582, 630, 638, 620, 416, 628, 400, 580, 440, 75, 636),
)
OWN_SEND = ((4, 5, 5, 4), (7, 5, 7, 7))
OWN_TAKE = ((4, 5, 5, 4), (7, 5, 7, 7))
LEAVES = (16, 8)
GATHER_TURN = 20
SCATTER_TURN = 28
GROUP = 4


def ring_kernel(n, envs, rows, a_hbm, f_ref, x_ref, r_ref, a_vmem, field, direction, image, sums,
           load_sem, send_sem, recv_sem, sum_send, sum_recv):
    order = ring_order(n)
    inverse = [order.index(i) for i in range(n)]
    me = lax.axis_index("dof")
    place = lookup(inverse, me)
    half = rows // 2
    far = n // 2
    tile = min(128, rows)

    def owner(step):
        return lookup(order, lax.rem(place + step + n, n))

    following, previous = owner(1), owner(-1)

    def load(env, block):
        return pltpu.make_async_copy(
            a_hbm.at[env, :, pl.ds(pl.multiple_of(block * rows, rows), rows)],
            a_vmem.at[env, block],
            load_sem.at[env, block],
        )

    def hop(env, way, block, part, target):
        return pltpu.make_async_remote_copy(
            src_ref=field.at[env, block, part],
            dst_ref=field.at[env, block, part],
            send_sem=send_sem.at[env, way, block, part],
            recv_sem=recv_sem.at[env, block, part],
            device_id={"dof": target},
            device_id_type=MESH,
        )

    def forward(env, block, part):
        return hop(env, 0, block, part, following)

    def backward(env, block, part):
        return hop(env, 1, block, part, previous)

    def share(env, slot, peer, source):
        return pltpu.make_async_remote_copy(
            src_ref=sums.at[env, slot, source],
            dst_ref=sums.at[env, slot, source],
            send_sem=sum_send.at[env, slot, peer],
            recv_sem=sum_recv.at[env, slot, source],
            device_id={"dof": peer},
            device_id_type=MESH,
        )

    def peer_of(j):
        return lax.rem(me + j, n)

    def add(env, block, part, first=False):
        product = jnp.dot(
            a_vmem[env, block, :, part * half:(part + 1) * half],
            field[env, block, part],
            preferred_element_type=jnp.float32,
        )
        if first:
            image[env] = product
        else:
            image[env] += product

    def start_own(env):
        for q in range(2):
            forward(env, me, q).start()
            backward(env, me, 1 - q).start()

    def begin(env, k):
        @pl.when(k == 0)
        def _():
            load(env, me).wait()
        add(env, me, 0, first=True)
        add(env, me, 1)

    def near(env, k, s, relay):
        before, after = owner(-s), owner(s)
        for q in range(2):
            forward(env, before, q).wait_recv()
            if relay > q:
                forward(env, before, q).start()
            backward(env, after, 1 - q).wait_recv()
            if relay > q:
                backward(env, after, 1 - q).start()
            if q == 0:
                @pl.when(k == 0)
                def _():
                    load(env, before).wait()
                    load(env, after).wait()
            if relay == 1 and q == 0:
                yield
            add(env, before, q)
            add(env, after, 1 - q)

    def gather(env, k, between):
        begin(env, k)

        def step(s, carry):
            for _ in near(env, k, s, 2):
                pass
            return carry

        lax.fori_loop(1, far - 1, step, 0)
        for _ in near(env, k, far - 1, 1):
            between()
        block = owner(far)
        forward(env, block, 0).wait_recv()

        @pl.when(k == 0)
        def _():
            load(env, block).wait()
        add(env, block, 0)
        backward(env, block, 1).wait_recv()
        add(env, block, 1)

        def drain(s, carry):
            for q in range(2):
                forward(env, owner(-s), q).wait_send()
                backward(env, owner(s), q).wait_send()
            return carry

        lax.fori_loop(0, far - 1, drain, 0)
        forward(env, owner(1 - far), 0).wait_send()
        backward(env, owner(far - 1), 1).wait_send()

    def local_sums(env, k):
        slot = lax.rem(k, 2)

        def step(i, carry):
            at = pl.ds(pl.multiple_of(i * tile, tile), tile)
            r, d, q = r_ref[env, at, :], direction[env, at, :], image[env, at, :]
            fold = lambda v: jnp.sum(v.reshape(tile // 8, 8, v.shape[-1]), axis=0)
            return tuple(c + fold(v) for c, v in zip(carry, (r * r, d * q, r * q, q * q)))

        zero = jnp.zeros((8, image.shape[-1]), jnp.float32)
        totals = lax.fori_loop(0, rows // tile, step, (zero,) * 4)
        for i, total in enumerate(totals):
            sums[env, slot, me, i:i + 1, :] = jnp.sum(total, axis=0, keepdims=True)

        def send(j, carry):
            share(env, slot, peer_of(j), me).start()
            return carry

        lax.fori_loop(1, n, send, 0)

    def update(env, k):
        slot = lax.rem(k, 2)

        def receive(j, carry):
            share(env, slot, me, peer_of(j)).wait_recv()
            share(env, slot, peer_of(j), me).wait_send()
            return carry

        lax.fori_loop(1, n, receive, 0)
        total = sums[env, slot, 0]
        for j in range(1, n):
            total = total + sums[env, slot, j]
        now, curve, cross, square = (total[i:i + 1, :] for i in range(4))
        alpha = now / curve
        beta = (now - 2.0 * alpha * cross + alpha * alpha * square) / now

        def step(i, carry):
            at = pl.ds(pl.multiple_of(i * tile, tile), tile)
            d = direction[env, at, :]
            x_ref[env, at, :] = x_ref[env, at, :] + alpha * d
            r = r_ref[env, at, :] - alpha * image[env, at, :]
            r_ref[env, at, :] = r
            d = r + beta * d
            direction[env, at, :] = d
            put(env, i, d)
            return carry

        lax.fori_loop(0, rows // tile, step, 0)

    def put(env, i, d):
        per = half // tile if half >= tile else 1
        narrow = d.astype(field.dtype)
        if half >= tile:
            at = pl.ds(pl.multiple_of(lax.rem(i, per) * tile, tile), tile)
            field[env, me, i // per, at, :] = narrow
        else:
            for q in range(2):
                field[env, me, q] = narrow[q * half:(q + 1) * half]

    barrier = pltpu.get_barrier_semaphore()

    def greet(j, carry):
        pl.semaphore_signal(barrier, inc=1, device_id={"dof": peer_of(j)}, device_id_type=MESH)
        return carry

    def copy_in(env):
        def step(i, carry):
            at = pl.ds(pl.multiple_of(i * tile, tile), tile)
            f = f_ref[env, at, :]
            x_ref[env, at, :] = jnp.zeros_like(f)
            r_ref[env, at, :] = f
            direction[env, at, :] = f
            put(env, i, f)
            return carry
        lax.fori_loop(0, rows // tile, step, 0)

    lax.fori_loop(1, n, greet, 0)
    copy_in(0)
    for env in range(envs):
        load(env, me).start()

        def fetch(s, carry):
            load(env, owner(-s)).start()
            load(env, owner(s)).start()
            return carry

        lax.fori_loop(1, far, fetch, 0)
        load(env, owner(far)).start()
    pl.semaphore_wait(barrier, n - 1)
    start_own(0)
    copy_in(1)

    def iteration(k, carry):
        def second():
            @pl.when(k > 0)
            def _():
                update(1, k - 1)
            start_own(1)

        def first():
            update(0, k)

            @pl.when(k < ITERS - 1)
            def _():
                start_own(0)

        gather(0, k, second)
        local_sums(0, k)
        gather(1, k, first)
        local_sums(1, k)
        return carry

    lax.fori_loop(0, ITERS, iteration, 0)
    update(1, ITERS - 1)


def ladder_kernel(n, depth, rows, a_hbm, f_ref, out, a_gather, a_scatter,
                  field, inbox, outbox, narrow, parts, xg, rg, dg, image, xs, rs, ds, drawn, sums,
                  load_sem, gather_send, gather_recv, scatter_send, scatter_recv, sum_send, sum_recv):
    width = 2
    rhs = image.shape[-1]
    piece = rows // PIECES
    tile = min(128, rows)
    me = lax.axis_index("dof")
    core = lax.rem(lax.axis_index("env"), 2)
    other = 1 - core
    x = lax.rem(me, width)
    z = me // width
    high = z // (depth // 2)
    place = z + high * (depth - 1 - 2 * z)
    inward = 1 - 2 * high
    targets = (me + 1 - 2 * x, me - width * inward, me + width * inward)
    near_slot, far_slot = (3 - inward) // 2, (3 + inward) // 2
    take_slot = (jnp.int32(0), near_slot, far_slot)
    give_slot = (jnp.int32(0), far_slot, near_slot)

    def by_place(pair):
        return jnp.where(place == 1, jnp.int32(pair[1]), jnp.int32(pair[0]))

    def node(r):
        level = r // width
        return (level + high * (depth - 1 - 2 * level)) * width + lax.rem(x + lax.rem(r, width), width)

    plans = [
        [by_place([t[i] + 1024 * t[i + 1] for t in tables]) for i in range(0, len(tables[0]), 2)]
        for tables in (GATHER, SCATTER)
    ]

    def read_plan(kind, pair):
        word = jnp.int32(0)
        for spot, value in enumerate(plans[kind]):
            word = word + jnp.where(pair == spot, value, jnp.int32(0))
        return [
            (node(lax.rem(entry, 8)), lax.rem(entry // 8, 4), lax.rem(entry // 32, 8), entry // 256)
            for entry in (lax.rem(word, 1024), word // 1024)
        ]

    def for_bits(mask, body):
        for d in range(3):
            @pl.when(lax.rem(mask // (1 << d), 2) == 1)
            def _(d=d):
                body(d)

    def load(kind, block, q):
        env, buffer = ((core, a_gather), (other, a_scatter))[kind]
        return pltpu.make_async_copy(
            a_hbm.at[env, :, pl.ds(pl.multiple_of(block * rows + q * piece, piece), piece)],
            buffer.at[block, q],
            load_sem.at[kind, block, q],
        )

    def spread(block, q, d, k):
        return pltpu.make_async_remote_copy(
            src_ref=field.at[lax.rem(k, 2), block, q],
            dst_ref=field.at[lax.rem(k, 2), block, q],
            send_sem=gather_send.at[block, q, d],
            recv_sem=gather_recv.at[block, q],
            device_id={"dof": targets[d]},
            device_id_type=MESH,
        )

    def collect(block, q, slot, target):
        return pltpu.make_async_remote_copy(
            src_ref=outbox.at[block, q],
            dst_ref=inbox.at[block, q, slot],
            send_sem=scatter_send.at[block, q],
            recv_sem=scatter_recv.at[block, q, slot],
            device_id={"dof": target},
            device_id_type=MESH,
        )

    def share(kind, peer, source):
        return pltpu.make_async_remote_copy(
            src_ref=sums.at[kind, source],
            dst_ref=sums.at[kind, source],
            send_sem=sum_send.at[kind, peer],
            recv_sem=sum_recv.at[kind, source],
            device_id={"dof": peer},
            device_id_type=MESH,
        )

    def peer_of(j):
        return lax.rem(me + j, n)

    def send_field(block, q, mask, k):
        def one(d):
            @pl.when(k > 0)
            def _():
                spread(block, q, d, k - 1).wait_send()
            spread(block, q, d, k).start()
        for_bits(mask, one)

    def gather_start(k):
        for q in range(PIECES):
            send_field(me, q, by_place([t[q] for t in OWN_SEND]), k)

    def loaded(kind, blocks, k):
        @pl.when(k == 0)
        def _():
            for block, q in blocks:
                load(kind, block, q).wait()

    def times(block, q, k):
        return jnp.dot(a_gather[block, q], field[lax.rem(k, 2), block, q], preferred_element_type=jnp.float32)

    def gather_own(k):
        loaded(0, [(me, q) for q in range(PIECES)], k)
        image[...] = functools.reduce(jnp.add, [times(me, q, k) for q in range(PIECES)])

    def gather_steps(lo, hi, k):
        def group(g, carry):
            blocks = []
            for j in range(GROUP // 2):
                for block, q, mask, _ in read_plan(0, g * (GROUP // 2) + j):
                    spread(block, q, 0, k).wait_recv()
                    send_field(block, q, mask, k)
                    blocks.append((block, q))
            loaded(0, blocks, k)
            products = [times(block, q, k) for block, q in blocks]
            image[...] += functools.reduce(jnp.add, products)
            return carry

        lax.fori_loop(lo // GROUP, hi // GROUP, group, 0)

    def gather_drain():
        for q in range(PIECES):
            for_bits(by_place([t[q] for t in OWN_SEND]), lambda d: spread(me, q, d, ITERS - 1).wait_send())

        def step(i, carry):
            for block, q, mask, _ in read_plan(0, i):
                for_bits(mask, lambda d: spread(block, q, d, ITERS - 1).wait_send())
            return carry

        lax.fori_loop(0, len(GATHER[0]) // 2, step, 0)

    def part(block, q):
        return jnp.dot(narrow[...], a_scatter[block, q], preferred_element_type=jnp.float32)

    def take(block, q, mask, total):
        def one(d):
            collect(block, q, take_slot[d], me).wait_recv()
            total[...] += inbox[block, q, take_slot[d]].astype(jnp.float32)
        for_bits(mask, one)

    def give(block, q, parent, value, k):
        @pl.when(k > 0)
        def _():
            collect(block, q, 0, targets[0]).wait_send()
        outbox[block, q] = value.astype(outbox.dtype)
        for d in range(3):
            @pl.when(parent == d)
            def _(d=d):
                collect(block, q, give_slot[d], targets[d]).start()

    def scatter_leaves(k):
        def group(g, carry):
            entries = read_plan(1, g)
            loaded(1, [(block, q) for block, q, _, _ in entries], k)
            values = [part(block, q) for block, q, _, _ in entries]
            for (block, q, _, parent), value in zip(entries, values):
                give(block, q, parent, value, k)
            return carry

        lax.fori_loop(0, leaves // 2, group, 0)

    def scatter_parts(k):
        def group(g, carry):
            entries = read_plan(1, g)
            loaded(1, [(block, q) for block, q, _, _ in entries], k)
            for j, (block, q, _, _) in enumerate(entries):
                parts[2 * g + j] = part(block, q)
            return carry

        lax.fori_loop(leaves // 2, len(SCATTER[0]) // 2, group, 0)
        loaded(1, [(me, q) for q in range(PIECES)], k)
        for q in range(PIECES):
            drawn[q] = part(me, q)

    def scatter_steps(lo, hi, k):
        def step(i, carry):
            for j, (block, q, mask, parent) in enumerate(read_plan(1, i)):
                take(block, q, mask, parts.at[2 * i + j])
                give(block, q, parent, parts[2 * i + j], k)
            return carry

        lax.fori_loop(lo // 2, hi // 2, step, 0)

    def scatter_own():
        for q in range(PIECES):
            take(me, q, by_place([t[q] for t in OWN_TAKE]), drawn.at[q])

    def scatter_drain():
        def step(i, carry):
            for block, q, _, _ in read_plan(1, i):
                collect(block, q, 0, targets[0]).wait_send()
            return carry

        lax.fori_loop(0, len(SCATTER[0]) // 2, step, 0)

    def send_sums(kind, rows_of):
        for i, total in enumerate(rows_of):
            sums[kind, me, i:i + 1, :] = total

        def send(j, carry):
            share(kind, peer_of(j), me).start()
            return carry

        lax.fori_loop(1, n, send, 0)

    def gather_sums():
        def step(i, carry):
            at = pl.ds(pl.multiple_of(i * tile, tile), tile)
            r, d, q = rg[at, :], dg[at, :], image[at, :]
            fold = lambda v: jnp.sum(v.reshape(tile // 8, 8, rhs), axis=0)
            return tuple(c + fold(v) for c, v in zip(carry, (r * r, d * q, r * q, q * q)))

        zero = jnp.zeros((8, rhs), jnp.float32)
        totals = lax.fori_loop(0, rows // tile, step, (zero,) * 4)
        send_sums(0, [jnp.sum(total, axis=0, keepdims=True) for total in totals])

    def cuts():
        for q in range(PIECES):
            for j in range(piece // rhs):
                yield q, slice(j * rhs, (j + 1) * rhs), q * piece + j * rhs

    def scatter_sums():
        totals = [jnp.zeros((rhs, rhs), jnp.float32)] * 4
        for q, lanes, _ in cuts():
            r, d, v = rs[q, :, lanes], ds[q, :, lanes], drawn[q, :, lanes]
            totals = [c + w for c, w in zip(totals, (r * r, d * v, r * v, v * v))]
        send_sums(1, [jnp.sum(total.T, axis=0, keepdims=True) for total in totals])

    def ratios(kind):
        def receive(j, carry):
            share(kind, me, peer_of(j)).wait_recv()
            share(kind, peer_of(j), me).wait_send()
            return carry

        lax.fori_loop(1, n, receive, 0)
        total = sums[kind, 0]
        for j in range(1, n):
            total = total + sums[kind, j]
        now, curve, cross, square = (total[i:i + 1, :] for i in range(4))
        alpha = now / curve
        beta = (now - 2.0 * alpha * cross + alpha * alpha * square) / now
        return alpha, beta

    def gather_update(later):
        alpha, beta = ratios(0)
        for q in range(PIECES):
            at = slice(q * piece, (q + 1) * piece)
            d = dg[at, :]
            xg[at, :] = xg[at, :] + alpha * d
            r = rg[at, :] - alpha * image[at, :]
            rg[at, :] = r
            d = r + beta * d
            dg[at, :] = d
            field[lax.rem(later, 2), me, q] = d.astype(field.dtype)

    def scatter_update():
        alpha, beta = (jnp.broadcast_to(v, (rhs, rhs)).T for v in ratios(1))
        for q, lanes, at in cuts():
            d = ds[q, :, lanes]
            xs[q, :, lanes] = xs[q, :, lanes] + alpha * d
            r = rs[q, :, lanes] - alpha * drawn[q, :, lanes]
            rs[q, :, lanes] = r
            d = r + beta * d
            ds[q, :, lanes] = d
            narrow[:, at:at + rhs] = d.astype(narrow.dtype)

    def strided(env, start, size):
        return pl.ds(env + 2 * start, size, stride=2)

    barrier = pltpu.get_barrier_semaphore()

    def greet(j, carry):
        pl.semaphore_signal(barrier, inc=1, device_id={"dof": peer_of(j)}, device_id_type=MESH)
        return carry

    lax.fori_loop(1, n, greet, 0)
    leaves = by_place(LEAVES)

    def fetch(kind, i):
        block = node(i if kind == 0 else n - 1 - i)
        for q in range(PIECES):
            load(kind, block, q).start()

    def fetch_all(first):
        def body(i, carry):
            fetch(first, i)
            return carry

        lax.fori_loop(0, n, body, 0)

    @pl.when(core == 0)
    def _():
        fetch_all(0)
        fetch_all(1)

    @pl.when(core == 1)
    def _():
        fetch_all(1)
        fetch_all(0)

    for q in range(PIECES):
        at = slice(q * piece, (q + 1) * piece)
        f = f_ref[strided(core, q * piece, piece), :]
        xg[at, :] = jnp.zeros_like(f)
        rg[at, :] = f
        dg[at, :] = f
        field[0, me, q] = f.astype(field.dtype)
    for q, lanes, at in cuts():
        f = f_ref[strided(other, at, rhs), :].T
        xs[q, :, lanes] = jnp.zeros_like(f)
        rs[q, :, lanes] = f
        ds[q, :, lanes] = f
        narrow[:, at:at + rhs] = f.astype(narrow.dtype)

    pl.semaphore_wait(barrier, n - 1)
    turns = 2 * ITERS

    @pl.when(core == 0)
    def _():
        gather_start(jnp.int32(0))
        gather_own(jnp.int32(0))

    @pl.when(core == 1)
    def _():
        scatter_leaves(jnp.int32(0))

    def phase(t, carry):
        k, later = t // 2, (t + 1) // 2
        kind = lax.rem(t + core, 2)

        @pl.when(kind == 0)
        def _():
            gather_steps(0, GATHER_TURN, k)

            @pl.when(t > 0)
            def _():
                scatter_update()

            @pl.when(t < turns - 1)
            def _():
                scatter_leaves(later)
            gather_steps(GATHER_TURN, len(GATHER[0]), k)
            gather_sums()

        @pl.when(kind == 1)
        def _():
            scatter_parts(k)
            scatter_steps(leaves, SCATTER_TURN, k)

            @pl.when(t > 0)
            def _():
                gather_update(later)

            @pl.when(t < turns - 1)
            def _():
                gather_start(later)
                gather_own(later)
            scatter_steps(SCATTER_TURN, len(SCATTER[0]), k)
            scatter_own()
            scatter_sums()
        return carry

    lax.fori_loop(0, turns, phase, 0)
    gather_drain()
    scatter_drain()

    @pl.when(core == 0)
    def _():
        scatter_update()

    @pl.when(core == 1)
    def _():
        gather_update(jnp.int32(ITERS))
    out[0, strided(core, 0, rows), :] = xg[...]
    out[1, strided(core, 0, rows), :] = rg[...]
    for q, lanes, at in cuts():
        out[0, strided(other, at, rhs), :] = xs[q, :, lanes].T
        out[1, strided(other, at, rhs), :] = rs[q, :, lanes].T


def ladder(n, depth, system_matrix, forces):
    envs, rows, _ = system_matrix.shape
    rhs = forces.shape[-1]
    piece = rows // PIECES
    both = jax.ShapeDtypeStruct((2, rows * envs, rhs), jnp.float32)
    vmem = pl.BlockSpec(memory_space=pltpu.VMEM)
    tall = pltpu.VMEM((rows, rhs), jnp.float32)
    wide = pltpu.VMEM((PIECES, rhs, piece), jnp.float32)
    out = pl.pallas_call(
        functools.partial(ladder_kernel, n, depth, rows),
        out_shape=both,
        in_specs=[pl.BlockSpec(memory_space=pl.ANY), vmem],
        out_specs=vmem,
        scratch_shapes=[
            pltpu.VMEM((n, PIECES, rows, piece), jnp.bfloat16),
            pltpu.VMEM((n, PIECES, rows, piece), jnp.bfloat16),
            pltpu.VMEM((2, n, PIECES, piece, rhs), jnp.bfloat16),
            pltpu.VMEM((n, PIECES, 3, rhs, piece), jnp.bfloat16),
            pltpu.VMEM((n, PIECES, rhs, piece), jnp.bfloat16),
            pltpu.VMEM((rhs, rows), jnp.bfloat16),
            pltpu.VMEM((len(SCATTER[0]), rhs, piece), jnp.float32),
            tall, tall, tall, tall,
            wide, wide, wide, wide,
            pltpu.VMEM((2, n, 4, rhs), jnp.float32),
            pltpu.SemaphoreType.DMA((2, n, PIECES)),
            pltpu.SemaphoreType.DMA((n, PIECES, 3)),
            pltpu.SemaphoreType.DMA((n, PIECES)),
            pltpu.SemaphoreType.DMA((n, PIECES)),
            pltpu.SemaphoreType.DMA((n, PIECES, 3)),
            pltpu.SemaphoreType.DMA((2, n)),
            pltpu.SemaphoreType.DMA((2, n)),
        ],
        compiler_params=pltpu.CompilerParams(
            collective_id=0, has_side_effects=True, vmem_limit_bytes=62 * 1024 * 1024
        ),
    )(system_matrix, forces.reshape(rows * envs, rhs))
    return out[0].reshape(rows, envs, rhs), out[1].reshape(rows, envs, rhs)


def ring(n, system_matrix, forces):
    envs, rows, _ = system_matrix.shape
    rhs = forces.shape[-1]
    block = jax.ShapeDtypeStruct((envs, rows, rhs), jnp.float32)
    vmem = pl.BlockSpec(memory_space=pltpu.VMEM)
    x, r = pl.pallas_call(
        functools.partial(ring_kernel, n, envs, rows),
        out_shape=(block, block),
        in_specs=[pl.BlockSpec(memory_space=pl.ANY), vmem],
        out_specs=(vmem, vmem),
        scratch_shapes=[
            pltpu.VMEM((envs, n, rows, rows), jnp.bfloat16),
            pltpu.VMEM((envs, n, 2, rows // 2, rhs), jnp.bfloat16),
            pltpu.VMEM((envs, rows, rhs), jnp.float32),
            pltpu.VMEM((envs, rows, rhs), jnp.float32),
            pltpu.VMEM((envs, 2, n, 4, rhs), jnp.float32),
            pltpu.SemaphoreType.DMA((envs, n)),
            pltpu.SemaphoreType.DMA((envs, 2, n, 2)),
            pltpu.SemaphoreType.DMA((envs, n, 2)),
            pltpu.SemaphoreType.DMA((envs, 2, n)),
            pltpu.SemaphoreType.DMA((envs, 2, n)),
        ],
        compiler_params=pltpu.CompilerParams(
            collective_id=0, has_side_effects=True, vmem_limit_bytes=60 * 1024 * 1024
        ),
    )(system_matrix, forces.transpose(1, 0, 2))
    return x.transpose(1, 0, 2), r.transpose(1, 0, 2)


def grid_of(n):
    width = 1
    while (2 * width) ** 2 <= n:
        width *= 2
    return width, n // width


def solution(mesh):
    n = mesh.shape["dof"]

    def on_device(system_matrix, forces):
        envs, rows, _ = system_matrix.shape
        rhs = forces.shape[-1]
        fits = envs == 2 and rhs == 128 and rows % (PIECES * rhs) == 0
        if grid_of(n) == LADDER and mesh.shape["env"] % 2 == 0 and fits:
            return ladder(n, LADDER[1], system_matrix, forces)
        return ring(n, system_matrix, forces)

    return jax.shard_map(
        on_device,
        mesh=mesh,
        in_specs=(P("env", "dof", None), P("dof", "env", None)),
        out_specs=(P("dof", "env", None), P("dof", "env", None)),
        check_vma=False,
    )
```
